32 devices in a mesh: gz: 16 (over z, y, x), ta: 2 (over core).
Axes of the slice: x: 2, y: 2, z: 4, core: 2. Of those that a mesh axis runs over, the one named last changes fastest.
Arguments:
- position: float32 [2, 48, 32, 512], P(None, 'gz', 'ta'), may hold values from -6 to 6
- gaps: float32 [2, 3, 48, 32, 512], P(None, None, 'gz', 'ta'), may hold values from -6 to 6
- weights: float32 [3, 48, 32, 512], P(None, 'gz', 'ta'), may hold values from 0.2 to 2
- deltas: int32 [3, 48, 32, 512], P(None, 'gz', 'ta'), may hold values from 0 to 8
- springs: int32 [2, 48, 32, 512], P(None, 'gz', 'ta'), may hold values 0 or 1
- damping: float32 [48, 32, 512], P('gz', 'ta'), may hold values from 0.1 to 1
- stiffness: float32 [2, 48], P(None, 'gz'), may hold values from 0.5 to 4
Outputs:
- update: float32 [2, 48, 32, 512], P(None, 'gz', 'ta')
- residual: float32 [2, 48, 32, 512], P(None, 'gz', 'ta')
The draws below stay inside these ranges and needn't reach their ends.
All inputs are finite; a program needn't handle non-finite values. No bound on the sum of `springs` on one device may be relied on, other than what follows from the above.
Results may differ from the reference program's by a relative error of at most 0.00012.
Values sent between devices are 32-bit elements; how exact they have to be, the bound alone decides.
A program may use at most 64 MiB of HBM per device.

```python
import math
import jax
import jax.numpy as jnp
from jax import lax

COLS = 512
ITERS = 2
SECTIONS = 48
ROWS = 32


def touch_ends(entries, key, least, high):
    longest = entries.shape.index(max(entries.shape))
    spots = []
    for shift in (0, 1):
        where = [jax.random.randint(jax.random.fold_in(key, axis), (), 0, length) for axis, length in enumerate(entries.shape)]
        where[longest] = (where[longest] + shift) % entries.shape[longest]
        spots.append(tuple(where))
    return entries.at[spots[0]].set(least).at[spots[1]].set(high)


def shard_levels(rng, dims, pieces, low, largest):
    def one(axis_at, blocks):
        steps = jax.random.uniform(jax.random.fold_in(jax.random.fold_in(rng, 6), axis_at), (blocks,), jnp.float32, low / len(pieces), largest / len(pieces))
        return jnp.repeat(jnp.exp(steps), dims[axis_at] // blocks).reshape((-1,) + (1,) * (len(dims) - axis_at - 1))

    loudness = one(*pieces[0])
    for cut in pieces[1:]:
        loudness = loudness * one(*cut)
    return loudness


def centred(stream_key, dims, width, most, pieces=(), kind=jnp.bfloat16):
    array = width * jax.random.normal(stream_key, dims, jnp.float32)
    if pieces:
        array = array * shard_levels(stream_key, dims, pieces, -0.22, 0.18)
    return jnp.clip(array, -most, most).astype(kind)


def setup_inputs(seed: int = 0) -> dict:
    streams_of = jax.random.split(jax.random.key(seed), 8)
    return {
        "position": centred(streams_of[0], (2, SECTIONS, ROWS, COLS), 1.0, 6.0, ((1, 16), (2, 2)), jnp.float32),
        "gaps": centred(streams_of[1], (2, 3, SECTIONS, ROWS, COLS), 1.0, 6.0, ((2, 16), (3, 2)), jnp.float32),
        "weights": jnp.clip(jnp.exp(math.log(2.0) - 2.3025851 * jax.random.uniform(streams_of[2], (3, SECTIONS, ROWS, COLS), jnp.float32) ** shard_levels(streams_of[2], (3, SECTIONS, ROWS, COLS), ((1, 16), (2, 2)), -0.2, 0.2)), 0.2, 2.0),
        "deltas": touch_ends(jax.random.randint(streams_of[3], (3, SECTIONS, ROWS, COLS), 0, 9), jax.random.fold_in(streams_of[3], 1), 0, 8).astype(jnp.int32),
        "springs": touch_ends((jax.random.randint(streams_of[4], (2, SECTIONS, ROWS, COLS), 0, 10) < 9).astype(jnp.int32), jax.random.fold_in(streams_of[4], 1), 0, 1),
        "damping": jnp.clip(jnp.exp(math.log(1.0) - 2.3025851 * jax.random.uniform(streams_of[5], (SECTIONS, ROWS, COLS), jnp.float32) ** shard_levels(streams_of[5], (SECTIONS, ROWS, COLS), ((0, 16), (1, 2)), -0.2, 0.2)), 0.1, 1.0),
        "stiffness": jnp.clip(jnp.exp(math.log(4.0) - 2.0794415 * jax.random.uniform(streams_of[6], (2, SECTIONS), jnp.float32) ** shard_levels(streams_of[6], (2, SECTIONS), ((1, 16),), -0.2, 0.2)), 0.5, 4.0),
    }


def shift_along(values, axis, step):
    if step == 0:
        return values
    length = values.shape[axis]
    widths = [(0, 0)] * values.ndim
    if step > 0:
        kept = lax.slice_in_dim(values, 0, length - step, axis=axis)
        widths[axis] = (step, 0)
    else:
        kept = lax.slice_in_dim(values, -step, length, axis=axis)
        widths[axis] = (0, -step)
    return jnp.pad(kept, widths)


def take_columns(field, delta):
    columns_at = lax.broadcasted_iota(jnp.int32, delta.shape, 2)
    index = jnp.clip(columns_at + delta - 4, 0, delta.shape[2] - 1).astype(jnp.int32)
    return jnp.take_along_axis(field, jnp.broadcast_to(index, field.shape), axis=3)


def column_valid(delta):
    columns_at = lax.broadcasted_iota(jnp.int32, delta.shape, 2)
    target = columns_at + delta - 4
    return jnp.where((target >= 0) & (target < delta.shape[2]), 1.0, 0.0).astype(jnp.float32)


def put_columns(values, delta):
    total = jnp.zeros_like(values)
    for place in range(9):
        total = total + shift_along(jnp.where(delta == place, values, 0.0), 3, place - 4)
    return total


def operator(field, gap_set, weights, deltas, springs, damping, stiffness):
    count, rows, cols = damping.shape
    sections_at = lax.broadcasted_iota(jnp.int32, (count, rows, cols), 0)
    rows_at = lax.broadcasted_iota(jnp.int32, (count, rows, cols), 1)
    columns_at = lax.broadcasted_iota(jnp.int32, (count, rows, cols), 2)
    along = stiffness[0][:, None, None]
    across = stiffness[1][:, None, None]
    horiz = jnp.where((springs[0] > 0) & (columns_at < cols - 1), 1.0, 0.0).astype(jnp.float32)
    vert = jnp.where((springs[1] > 0) & (rows_at < rows - 1), 1.0, 0.0).astype(jnp.float32)
    h_flux = along * horiz * (shift_along(field, 3, -1) - field)
    v_flux = across * vert * (shift_along(field, 2, -1) - field)
    total = damping * field - h_flux + shift_along(h_flux, 3, 1) - v_flux + shift_along(v_flux, 2, 1)
    for slot in range(3):
        offset = slot + 1
        partner = take_columns(shift_along(field, 1, -offset), deltas[slot])
        inside = jnp.where(sections_at + offset < count, 1.0, 0.0).astype(jnp.float32)
        strength = weights[slot] * column_valid(deltas[slot]) * inside
        mismatch = field - partner
        if gap_set is not None:
            mismatch = mismatch - gap_set[:, slot]
        pulled = strength * mismatch
        total = total + pulled - shift_along(put_columns(pulled, deltas[slot]), 1, offset)
    return total


def reference(position, gaps, weights, deltas, springs, damping, stiffness):
    rhs = -operator(position, gaps, weights, deltas, springs, damping, stiffness)
    update = jnp.zeros_like(rhs)
    residual = rhs
    direction = rhs
    norm_now = jnp.sum(residual * residual)
    for step in range(ITERS):
        image = operator(direction, None, weights, deltas, springs, damping, stiffness)
        alpha = norm_now / jnp.sum(direction * image)
        update = update + alpha * direction
        residual = residual - alpha * image
        norm_next = jnp.sum(residual * residual)
        direction = residual + (norm_next / norm_now) * direction
        norm_now = norm_next
    return update, residual
```

```python
import functools

import jax
import jax.numpy as jnp
from jax import lax
from jax.experimental import pallas as pl
from jax.experimental.pallas import tpu as pltpu
from jax.sharding import PartitionSpec as P

MESH = pl.DeviceIdType.MESH
PLACES = 9
HALF = 8
OPS = 3


def rolled(values, step):
    axis = values.ndim - 1
    return values if step == 0 else pltpu.roll(values, step % values.shape[axis], axis)


def kernel(
    n, pos_h, gaps_h, wei_h, del_h, spr_h, dam_h, stiff,
    upd, res,
    v, up, tsend, trecv, esend, erecv, sall, gath,
    gaps, wei, dlt, spr, dam, vc, hc, hl, diag, qbuf,
    load_sem, vs_sem, vr_sem, ts_sem, tr_sem, es_sem, er_sem, gs_sem, gr_sem,
):
    g = lax.axis_index("gz")
    t = lax.axis_index("ta")
    secs, rows, cols = dam_h.shape
    chunks = rows // HALF
    other = {"gz": g, "ta": 1 - t}
    lower = {"gz": g - 1, "ta": t}
    upper = {"gz": g + 1, "ta": t}
    has_lower = g > 0
    has_upper = g < n - 1
    base = HALF

    loads = [
        pltpu.make_async_copy(pos_h, v.at[0, :, :, pl.ds(base, rows)], load_sem.at[0]),
        pltpu.make_async_copy(del_h, dlt, load_sem.at[1]),
        pltpu.make_async_copy(wei_h, wei, load_sem.at[2]),
        pltpu.make_async_copy(gaps_h, gaps, load_sem.at[3]),
        pltpu.make_async_copy(spr_h, spr, load_sem.at[4]),
        pltpu.make_async_copy(dam_h, dam, load_sem.at[5]),
    ]
    for load in loads:
        load.start()

    barrier = pltpu.get_barrier_semaphore()
    pl.semaphore_signal(barrier, inc=1, device_id=other, device_id_type=MESH)
    for j in range(1, n):
        pl.semaphore_signal(
            barrier, inc=1, device_id={"gz": lax.rem(g + j, n), "ta": t}, device_id_type=MESH
        )

    @pl.when(jnp.logical_not(has_upper))
    def _():
        up[...] = jnp.zeros_like(up)

    @pl.when(jnp.logical_not(has_lower))
    def _():
        trecv[...] = jnp.zeros_like(trecv)

    esend[...] = jnp.zeros_like(esend)

    def rows_at(h):
        return pl.ds(h * HALF, HALF)

    def v_copy(op, h):
        return pltpu.make_async_remote_copy(
            v.at[op, :, :, pl.ds(base + h * HALF, HALF)], up.at[op, :, :, rows_at(h)],
            vs_sem.at[op, h], vr_sem.at[op, h], device_id=lower, device_id_type=MESH,
        )

    def comps(op):
        return 3 if op == 0 else 2

    def t_copy(op, h):
        part = pl.ds(0, comps(op))
        return pltpu.make_async_remote_copy(
            tsend.at[op, part, :, rows_at(h)], trecv.at[op, part, :, rows_at(h)],
            ts_sem.at[op, h], tr_sem.at[op, h], device_id=upper, device_id_type=MESH,
        )

    def e_copy(op):
        return pltpu.make_async_remote_copy(
            esend.at[op], erecv.at[op], es_sem.at[op], er_sem.at[op],
            device_id=other, device_id_type=MESH,
        )

    def send_edges(op):
        for comp in range(2):
            for z in range(secs):
                top = v[op, comp, z, base : base + 1, :]
                bottom = v[op, comp, z, base + rows - 1 : base + rows, :]
                k = comp * secs + z
                esend[op, k : k + 1, :] = jnp.where(t == 0, bottom, top)
        if op == 0:
            for z in range(secs):
                k = 2 * secs + z
                esend[op, k : k + 1, :] = jnp.where(
                    spr[1, z, rows - 1 : rows, :] > 0, 1.0, 0.0
                ).astype(jnp.float32)
        e_copy(op).start()

    def take_edges(op):
        e_copy(op).wait_recv()
        for comp in range(2):
            for z in range(secs):
                k = comp * secs + z
                row = erecv[op, k : k + 1, :]
                v[op, comp, z, base - 1 : base, :] = jnp.where(t == 1, row, 0.0)
                v[op, comp, z, base + rows : base + rows + 1, :] = jnp.where(t == 0, row, 0.0)
        if op == 0:
            for z in range(secs):
                k = 2 * secs + z
                row = stiff[1, z] * erecv[op, k : k + 1, :]
                vc[z, base - 1 : base, :] = jnp.where(t == 1, row, 0.0)

    def scatter(op, h, dest):
        sources = [(dest - k - 1, k) for k in range(3) if 0 <= dest - k - 1 < secs]
        terms = []
        for z, k in sources:
            w = wei[k, z, rows_at(h)]
            field = v[op, :, z, pl.ds(base + h * HALF, HALF)]
            if op == 0:
                field = field - gaps[:, k, z, rows_at(h)]
                u = jnp.concatenate([w[None] * field, w[None]], 0)
            else:
                u = w[None] * field
            terms.append((dlt[k, z, rows_at(h)], u))
        total = None
        for place in range(PLACES):
            part = None
            for d, u in terms:
                one = jnp.where((d == place)[None], u, 0.0)
                part = one if part is None else part + one
            part = rolled(part, place - 4)
            total = part if total is None else total + part
        return total

    def send_up(op, h):
        for d in range(secs):
            tsend[op, pl.ds(0, comps(op)), d, rows_at(h)] = scatter(op, h, secs + d)

        @pl.when(has_upper)
        def _():
            t_copy(op, h).start()

    def send_down(op, h):
        @pl.when(has_lower)
        def _():
            v_copy(op, h).start()

    loads[0].wait()
    pl.semaphore_wait(barrier, n)
    for h in range(chunks):
        send_down(0, h)

    loads[1].wait()
    loads[2].wait()
    shape = (HALF, cols)
    columns_at = lax.broadcasted_iota(jnp.int32, shape, 1)
    row_at = lax.broadcasted_iota(jnp.int32, shape, 0)
    for k in range(3):
        for z in range(secs):
            inside = jnp.where(g * secs + z + k + 1 < n * secs, 1.0, 0.0).astype(jnp.float32)
            for h in range(chunks):
                target = columns_at + dlt[k, z, rows_at(h)] - 4
                valid = (target >= 0) & (target < cols)
                wei[k, z, rows_at(h)] = jnp.where(valid, wei[k, z, rows_at(h)], 0.0) * inside
    loads[3].wait()
    for h in range(chunks):
        send_up(0, h)
    loads[4].wait()
    send_edges(0)
    loads[5].wait()
    vc[...] = jnp.zeros_like(vc)
    for z in range(secs):
        for h in range(chunks):
            last = jnp.where((t == 1) & (row_at == HALF - 1), 0.0, 1.0) if h == chunks - 1 else 1.0
            vc[z, pl.ds(base + h * HALF, HALF)] = (
                stiff[1, z] * jnp.where(spr[1, z, rows_at(h)] > 0, 1.0, 0.0).astype(jnp.float32) * last
            )
            right = stiff[0, z] * jnp.where(
                (spr[0, z, rows_at(h)] > 0) & (columns_at < cols - 1), 1.0, 0.0
            ).astype(jnp.float32)
            hc[z, rows_at(h)] = right
            left = rolled(right, 1)
            hl[z, rows_at(h)] = left
            total = dam[z, rows_at(h)] + right + left
            for k in range(3):
                total = total + wei[k, z, rows_at(h)]
            diag[z, rows_at(h)] = total

    def local(op, h, write):
        here = pl.ds(base + h * HALF, HALF)
        own = {}
        for d in range(1, secs):
            own[d] = scatter(op, h, d)
            if op == 0:
                diag[d, rows_at(h)] = diag[d, rows_at(h)] + own[d][2]
        acc = [None] * secs
        for z in range(secs):
            center = v[op, :, z, here]
            acc[z] = -(
                hc[z, rows_at(h)][None] * rolled(center, -1)
                + hl[z, rows_at(h)][None] * rolled(center, 1)
            )
            if z > 0:
                acc[z] = acc[z] - own[z][0:2]
            if op == 0:
                for k in range(3):
                    acc[z] = acc[z] - wei[k, z, rows_at(h)][None] * gaps[:, k, z, rows_at(h)]

        def gather(s):
            field = v[op, :, s, here] if s < secs else up[op, :, s - secs, rows_at(h)]
            sources = [(s - k - 1, k) for k in range(3) if 0 <= s - k - 1 < secs]
            got = [None] * len(sources)
            for place in range(PLACES):
                moved = rolled(field, 4 - place)
                for i, (z, k) in enumerate(sources):
                    if got[i] is None:
                        got[i] = moved
                    else:
                        got[i] = jnp.where((dlt[k, z, rows_at(h)] == place)[None], moved, got[i])
            for i, (z, k) in enumerate(sources):
                acc[z] = acc[z] - wei[k, z, rows_at(h)][None] * got[i]

        for s in range(1, secs):
            gather(s)
        if h == 0:
            take_edges(op)
        for z in range(secs):
            if op == 0:
                above = vc[z, base + h * HALF - 1 : base + h * HALF - 1 + HALF, :]
                diag[z, rows_at(h)] = diag[z, rows_at(h)] + vc[z, here] + above
            first = base + h * HALF
            acc[z] = acc[z] - (
                vc[z, here][None] * v[op, :, z, first + 1 : first + 1 + HALF, :]
                + vc[z, first - 1 : first - 1 + HALF, :][None]
                * v[op, :, z, first - 1 : first - 1 + HALF, :]
            )

        @pl.when(has_lower)
        def _():
            t_copy(op, h).wait_recv()

        @pl.when(has_upper)
        def _():
            v_copy(op, h).wait_recv()

        for s in range(secs, 2 * secs):
            gather(s)
        for z in range(secs):
            if op == 0:
                diag[z, rows_at(h)] = diag[z, rows_at(h)] + trecv[op, 2, z, rows_at(h)]
            image = (
                acc[z]
                + diag[z, rows_at(h)][None] * v[op, :, z, here]
                - trecv[op, 0:2, z, rows_at(h)]
            )
            write(z, image)

    dots = [jnp.zeros(shape, jnp.float32) for _ in range(4)]

    def dot_into(i, a, b):
        dots[i] = dots[i] + a[0] * b[0] + a[1] * b[1]

    for op in range(OPS):
        for h in range(chunks):
            here = pl.ds(base + h * HALF, HALF)

            def write(z, image, op=op, h=h, here=here):
                if op == 0:
                    v[1, :, z, here] = -image
                    dot_into(0, image, image)
                elif op == 1:
                    v[2, :, z, here] = image
                    dot_into(1, v[1, :, z, here], image)
                    dot_into(2, image, image)
                else:
                    qbuf[:, z, rows_at(h)] = image
                    dot_into(3, v[2, :, z, here], image)

            local(op, h, write)
            if op + 1 < OPS:
                send_down(op + 1, h)
                send_up(op + 1, h)
        if op + 1 < OPS:
            send_edges(op + 1)

    lanes = 128
    packed = jnp.zeros((8, lanes), jnp.float32)
    sub = lax.broadcasted_iota(jnp.int32, (8, lanes), 0)
    for i in range(4):
        row = jnp.sum(dots[i], axis=0, keepdims=True)
        part = row[:, 0:lanes]
        for c in range(lanes, cols, lanes):
            part = part + row[:, c : c + lanes]
        packed = jnp.where(sub == i, part, packed)
    esend[OPS, 0:8, 0:lanes] = packed
    e_copy(OPS).start()
    e_copy(OPS).wait_recv()
    packed = packed + erecv[OPS, 0:8, 0:lanes]
    sall[...] = packed
    pushes = []
    for j in range(1, n):
        pushes.append(
            pltpu.make_async_remote_copy(
                sall, gath.at[j - 1], gs_sem.at[j - 1], gr_sem.at[j - 1],
                device_id={"gz": lax.rem(g + j, n), "ta": t}, device_id_type=MESH,
            )
        )
    for push in pushes:
        push.start()
    for push in pushes:
        push.wait_recv()
    total = packed
    for j in range(1, n):
        total = total + gath[j - 1]
    total = jnp.sum(total, axis=1, keepdims=True)
    rr, rm, mm, mq = (total[i : i + 1, :] for i in range(4))
    alpha0 = rr / rm
    rr1 = alpha0 * (alpha0 * mm) - rr
    ratio = rr1 / rr
    one = 1.0 + ratio
    curve = one * one * rm - 2.0 * one * alpha0 * mm + alpha0 * alpha0 * mq
    alpha1 = rr1 / curve
    for z in range(secs):
        for h in range(chunks):
            here = pl.ds(base + h * HALF, HALF)
            for comp in range(2):
                r0 = v[1, comp, z, here]
                m0 = v[2, comp, z, here]
                q = qbuf[comp, z, rows_at(h)]
                r1 = r0 - alpha0 * m0
                upd[comp, z, rows_at(h)] = alpha0 * r0 + alpha1 * (r1 + ratio * r0)
                res[comp, z, rows_at(h)] = r1 - alpha1 * (one * m0 - alpha0 * q)

    for push in pushes:
        push.wait_send()
    for op in range(OPS + 1):
        e_copy(op).wait_send()

    @pl.when(has_lower)
    def _():
        for op in range(OPS):
            for h in range(chunks):
                v_copy(op, h).wait_send()

    @pl.when(has_upper)
    def _():
        for op in range(OPS):
            for h in range(chunks):
                t_copy(op, h).wait_send()


def body(position, gaps, weights, deltas, springs, damping, stiffness):
    secs, rows, cols = damping.shape
    n = lax.axis_size("gz")
    chunks = rows // HALF
    f32, i32 = jnp.float32, jnp.int32
    edge = -(-3 * secs // 8) * 8
    padded = rows + 2 * HALF
    dma = pltpu.SemaphoreType.DMA
    out = jax.ShapeDtypeStruct(position.shape, f32)
    anyspace = pl.BlockSpec(memory_space=pl.ANY)
    vmem = pl.BlockSpec(memory_space=pltpu.VMEM)
    return pl.pallas_call(
        functools.partial(kernel, n),
        out_shape=(out, out),
        in_specs=[anyspace] * 6 + [pl.BlockSpec(memory_space=pltpu.SMEM)],
        out_specs=(vmem, vmem),
        scratch_shapes=[
            pltpu.VMEM((OPS, 2, secs, padded, cols), f32),
            pltpu.VMEM((OPS, 2, secs, rows, cols), f32),
            pltpu.VMEM((OPS, 3, secs, rows, cols), f32),
            pltpu.VMEM((OPS, 3, secs, rows, cols), f32),
            pltpu.VMEM((OPS + 1, edge, cols), f32),
            pltpu.VMEM((OPS + 1, edge, cols), f32),
            pltpu.VMEM((8, 128), f32),
            pltpu.VMEM((n - 1, 8, 128), f32),
            pltpu.VMEM(gaps.shape, f32),
            pltpu.VMEM(weights.shape, f32),
            pltpu.VMEM(deltas.shape, i32),
            pltpu.VMEM(springs.shape, i32),
            pltpu.VMEM(damping.shape, f32),
            pltpu.VMEM((secs, padded, cols), f32),
            pltpu.VMEM(damping.shape, f32),
            pltpu.VMEM(damping.shape, f32),
            pltpu.VMEM(damping.shape, f32),
            pltpu.VMEM(position.shape, f32),
            dma((6,)),
            dma((OPS, chunks)), dma((OPS, chunks)),
            dma((OPS, chunks)), dma((OPS, chunks)),
            dma((OPS + 1,)), dma((OPS + 1,)),
            dma((n - 1,)), dma((n - 1,)),
        ],
        compiler_params=pltpu.CompilerParams(
            collective_id=0, has_side_effects=True, vmem_limit_bytes=48 * 2**20
        ),
    )(position, gaps, weights, deltas, springs, damping, stiffness)


def solution(mesh):
    return jax.shard_map(
        body,
        mesh=mesh,
        in_specs=(
            P(None, "gz", "ta", None),
            P(None, None, "gz", "ta", None),
            P(None, "gz", "ta", None),
            P(None, "gz", "ta", None),
            P(None, "gz", "ta", None),
            P("gz", "ta", None),
            P(None, "gz"),
        ),
        out_specs=(P(None, "gz", "ta", None), P(None, "gz", "ta", None)),
        check_vma=False,
    )
```

```python
import functools

import jax
import jax.numpy as jnp
from jax import lax
from jax.experimental import pallas as pl
from jax.experimental.pallas import tpu as pltpu
from jax.sharding import PartitionSpec as P

MESH = pl.DeviceIdType.MESH
PLACES = 9
HALF = 8
OPS = 3


def rolled(values, step):
    axis = values.ndim - 1
    return values if step == 0 else pltpu.roll(values, step % values.shape[axis], axis)


def kernel(
    n, pos_h, gaps_h, wei_h, del_h, spr_h, dam_h, stiff,
    upd, res,
    v, up, tsend, trecv, esend, erecv, sall, gath,
    gaps, wei, dlt, spr, dam, vc, hc, hl, diag, qbuf,
    load_sem, vs_sem, vr_sem, ts_sem, tr_sem, es_sem, er_sem, gs_sem, gr_sem,
):
    g = lax.axis_index("gz")
    t = lax.axis_index("ta")
    secs, rows, cols = dam_h.shape
    chunks = rows // HALF
    other = {"gz": g, "ta": 1 - t}
    lower = {"gz": g - 1, "ta": t}
    upper = {"gz": g + 1, "ta": t}
    has_lower = g > 0
    has_upper = g < n - 1
    base = HALF

    loads = [
        pltpu.make_async_copy(pos_h, v.at[0, :, :, pl.ds(base, rows)], load_sem.at[0]),
        pltpu.make_async_copy(del_h, dlt, load_sem.at[1]),
        pltpu.make_async_copy(wei_h, wei, load_sem.at[2]),
        pltpu.make_async_copy(gaps_h, gaps, load_sem.at[3]),
        pltpu.make_async_copy(spr_h, spr, load_sem.at[4]),
        pltpu.make_async_copy(dam_h, dam, load_sem.at[5]),
    ]
    for load in loads:
        load.start()

    barrier = pltpu.get_barrier_semaphore()
    pl.semaphore_signal(barrier, inc=1, device_id=other, device_id_type=MESH)
    for j in range(1, n):
        pl.semaphore_signal(
            barrier, inc=1, device_id={"gz": lax.rem(g + j, n), "ta": t}, device_id_type=MESH
        )

    @pl.when(jnp.logical_not(has_upper))
    def _():
        up[...] = jnp.zeros_like(up)

    @pl.when(jnp.logical_not(has_lower))
    def _():
        trecv[...] = jnp.zeros_like(trecv)

    esend[...] = jnp.zeros_like(esend)

    def rows_at(h):
        return pl.ds(h * HALF, HALF)

    def v_copy(op, h):
        return pltpu.make_async_remote_copy(
            v.at[op, :, :, pl.ds(base + h * HALF, HALF)], up.at[op, :, :, rows_at(h)],
            vs_sem.at[op, h], vr_sem.at[op, h], device_id=lower, device_id_type=MESH,
        )

    def comps(op):
        return 3 if op == 0 else 2

    def t_copy(op, h):
        part = pl.ds(0, comps(op))
        return pltpu.make_async_remote_copy(
            tsend.at[op, part, :, rows_at(h)], trecv.at[op, part, :, rows_at(h)],
            ts_sem.at[op, h], tr_sem.at[op, h], device_id=upper, device_id_type=MESH,
        )

    def e_copy(op):
        return pltpu.make_async_remote_copy(
            esend.at[op], erecv.at[op], es_sem.at[op], er_sem.at[op],
            device_id=other, device_id_type=MESH,
        )

    def send_edges(op):
        for comp in range(2):
            for z in range(secs):
                top = v[op, comp, z, base : base + 1, :]
                bottom = v[op, comp, z, base + rows - 1 : base + rows, :]
                k = comp * secs + z
                esend[op, k : k + 1, :] = jnp.where(t == 0, bottom, top)
        if op == 0:
            for z in range(secs):
                k = 2 * secs + z
                esend[op, k : k + 1, :] = jnp.where(
                    spr[1, z, rows - 1 : rows, :] > 0, 1.0, 0.0
                ).astype(jnp.float32)
        e_copy(op).start()

    def take_edges(op):
        e_copy(op).wait_recv()
        for comp in range(2):
            for z in range(secs):
                k = comp * secs + z
                row = erecv[op, k : k + 1, :]
                v[op, comp, z, base - 1 : base, :] = jnp.where(t == 1, row, 0.0)
                v[op, comp, z, base + rows : base + rows + 1, :] = jnp.where(t == 0, row, 0.0)
        if op == 0:
            for z in range(secs):
                k = 2 * secs + z
                row = stiff[1, z] * erecv[op, k : k + 1, :]
                vc[z, base - 1 : base, :] = jnp.where(t == 1, row, 0.0)

    def scatter(op, h, dest):
        sources = [(dest - k - 1, k) for k in range(3) if 0 <= dest - k - 1 < secs]
        terms = []
        for z, k in sources:
            w = wei[k, z, rows_at(h)]
            field = v[op, :, z, pl.ds(base + h * HALF, HALF)]
            if op == 0:
                field = field - gaps[:, k, z, rows_at(h)]
                u = jnp.concatenate([w[None] * field, w[None]], 0)
            else:
                u = w[None] * field
            terms.append((dlt[k, z, rows_at(h)], u))
        total = None
        for place in range(PLACES):
            part = None
            for d, u in terms:
                one = jnp.where((d == place)[None], u, 0.0)
                part = one if part is None else part + one
            part = rolled(part, place - 4)
            total = part if total is None else total + part
        return total

    def send_up(op, h):
        for d in range(secs):
            tsend[op, pl.ds(0, comps(op)), d, rows_at(h)] = scatter(op, h, secs + d)

        @pl.when(has_upper)
        def _():
            t_copy(op, h).start()

    def send_down(op, h):
        @pl.when(has_lower)
        def _():
            v_copy(op, h).start()

    loads[0].wait()
    pl.semaphore_wait(barrier, n)
    send_down(0, 0)

    loads[1].wait()
    loads[2].wait()
    shape = (HALF, cols)
    columns_at = lax.broadcasted_iota(jnp.int32, shape, 1)
    row_at = lax.broadcasted_iota(jnp.int32, shape, 0)
    for k in range(3):
        for z in range(secs):
            inside = jnp.where(g * secs + z + k + 1 < n * secs, 1.0, 0.0).astype(jnp.float32)
            for h in range(chunks):
                target = columns_at + dlt[k, z, rows_at(h)] - 4
                valid = (target >= 0) & (target < cols)
                wei[k, z, rows_at(h)] = jnp.where(valid, wei[k, z, rows_at(h)], 0.0) * inside
    loads[3].wait()
    for h in range(chunks):
        send_up(0, h)
        if h + 1 < chunks:
            send_down(0, h + 1)
    loads[4].wait()
    send_edges(0)
    loads[5].wait()
    vc[...] = jnp.zeros_like(vc)
    for z in range(secs):
        for h in range(chunks):
            last = jnp.where((t == 1) & (row_at == HALF - 1), 0.0, 1.0) if h == chunks - 1 else 1.0
            vc[z, pl.ds(base + h * HALF, HALF)] = (
                stiff[1, z] * jnp.where(spr[1, z, rows_at(h)] > 0, 1.0, 0.0).astype(jnp.float32) * last
            )
            right = stiff[0, z] * jnp.where(
                (spr[0, z, rows_at(h)] > 0) & (columns_at < cols - 1), 1.0, 0.0
            ).astype(jnp.float32)
            hc[z, rows_at(h)] = right
            left = rolled(right, 1)
            hl[z, rows_at(h)] = left
            total = dam[z, rows_at(h)] + right + left
            for k in range(3):
                total = total + wei[k, z, rows_at(h)]
            diag[z, rows_at(h)] = total

    def local(op, h, write):
        here = pl.ds(base + h * HALF, HALF)
        own = {}
        for d in range(1, secs):
            own[d] = scatter(op, h, d)
            if op == 0:
                diag[d, rows_at(h)] = diag[d, rows_at(h)] + own[d][2]
        acc = [None] * secs
        for z in range(secs):
            center = v[op, :, z, here]
            acc[z] = -(
                hc[z, rows_at(h)][None] * rolled(center, -1)
                + hl[z, rows_at(h)][None] * rolled(center, 1)
            )
            if z > 0:
                acc[z] = acc[z] - own[z][0:2]
            if op == 0:
                for k in range(3):
                    acc[z] = acc[z] - wei[k, z, rows_at(h)][None] * gaps[:, k, z, rows_at(h)]

        def gather(s):
            field = v[op, :, s, here] if s < secs else up[op, :, s - secs, rows_at(h)]
            sources = [(s - k - 1, k) for k in range(3) if 0 <= s - k - 1 < secs]
            got = [None] * len(sources)
            for place in range(PLACES):
                moved = rolled(field, 4 - place)
                for i, (z, k) in enumerate(sources):
                    if got[i] is None:
                        got[i] = moved
                    else:
                        got[i] = jnp.where((dlt[k, z, rows_at(h)] == place)[None], moved, got[i])
            for i, (z, k) in enumerate(sources):
                acc[z] = acc[z] - wei[k, z, rows_at(h)][None] * got[i]

        for s in range(1, secs):
            gather(s)
        if h == 0:
            take_edges(op)
        for z in range(secs):
            if op == 0:
                above = vc[z, base + h * HALF - 1 : base + h * HALF - 1 + HALF, :]
                diag[z, rows_at(h)] = diag[z, rows_at(h)] + vc[z, here] + above
            first = base + h * HALF
            acc[z] = acc[z] - (
                vc[z, here][None] * v[op, :, z, first + 1 : first + 1 + HALF, :]
                + vc[z, first - 1 : first - 1 + HALF, :][None]
                * v[op, :, z, first - 1 : first - 1 + HALF, :]
            )

        @pl.when(has_lower)
        def _():
            t_copy(op, h).wait_recv()

        @pl.when(has_upper)
        def _():
            v_copy(op, h).wait_recv()

        for s in range(secs, 2 * secs):
            gather(s)
        for z in range(secs):
            if op == 0:
                diag[z, rows_at(h)] = diag[z, rows_at(h)] + trecv[op, 2, z, rows_at(h)]
            image = (
                acc[z]
                + diag[z, rows_at(h)][None] * v[op, :, z, here]
                - trecv[op, 0:2, z, rows_at(h)]
            )
            write(z, image)

    dots = [jnp.zeros(shape, jnp.float32) for _ in range(4)]

    def dot_into(i, a, b):
        dots[i] = dots[i] + a[0] * b[0] + a[1] * b[1]

    for op in range(OPS):
        for h in range(chunks):
            here = pl.ds(base + h * HALF, HALF)

            def write(z, image, op=op, h=h, here=here):
                if op == 0:
                    v[1, :, z, here] = -image
                    dot_into(0, image, image)
                elif op == 1:
                    v[2, :, z, here] = image
                    dot_into(1, v[1, :, z, here], image)
                    dot_into(2, image, image)
                else:
                    qbuf[:, z, rows_at(h)] = image
                    dot_into(3, v[2, :, z, here], image)

            local(op, h, write)
            if op + 1 < OPS:
                send_down(op + 1, h)
                send_up(op + 1, h)
        if op + 1 < OPS:
            send_edges(op + 1)

    lanes = 128
    packed = jnp.zeros((8, lanes), jnp.float32)
    sub = lax.broadcasted_iota(jnp.int32, (8, lanes), 0)
    for i in range(4):
        row = jnp.sum(dots[i], axis=0, keepdims=True)
        part = row[:, 0:lanes]
        for c in range(lanes, cols, lanes):
            part = part + row[:, c : c + lanes]
        packed = jnp.where(sub == i, part, packed)
    esend[OPS, 0:8, 0:lanes] = packed
    e_copy(OPS).start()
    e_copy(OPS).wait_recv()
    packed = packed + erecv[OPS, 0:8, 0:lanes]
    sall[...] = packed
    pushes = []
    for j in range(1, n):
        pushes.append(
            pltpu.make_async_remote_copy(
                sall, gath.at[j - 1], gs_sem.at[j - 1], gr_sem.at[j - 1],
                device_id={"gz": lax.rem(g + j, n), "ta": t}, device_id_type=MESH,
            )
        )
    for push in pushes:
        push.start()
    for push in pushes:
        push.wait_recv()
    total = packed
    for j in range(1, n):
        total = total + gath[j - 1]
    total = jnp.sum(total, axis=1, keepdims=True)
    rr, rm, mm, mq = (total[i : i + 1, :] for i in range(4))
    alpha0 = rr / rm
    rr1 = alpha0 * (alpha0 * mm) - rr
    ratio = rr1 / rr
    one = 1.0 + ratio
    curve = one * one * rm - 2.0 * one * alpha0 * mm + alpha0 * alpha0 * mq
    alpha1 = rr1 / curve
    for z in range(secs):
        for h in range(chunks):
            here = pl.ds(base + h * HALF, HALF)
            for comp in range(2):
                r0 = v[1, comp, z, here]
                m0 = v[2, comp, z, here]
                q = qbuf[comp, z, rows_at(h)]
                r1 = r0 - alpha0 * m0
                upd[comp, z, rows_at(h)] = alpha0 * r0 + alpha1 * (r1 + ratio * r0)
                res[comp, z, rows_at(h)] = r1 - alpha1 * (one * m0 - alpha0 * q)

    for push in pushes:
        push.wait_send()
    for op in range(OPS + 1):
        e_copy(op).wait_send()

    @pl.when(has_lower)
    def _():
        for op in range(OPS):
            for h in range(chunks):
                v_copy(op, h).wait_send()

    @pl.when(has_upper)
    def _():
        for op in range(OPS):
            for h in range(chunks):
                t_copy(op, h).wait_send()


def body(position, gaps, weights, deltas, springs, damping, stiffness):
    secs, rows, cols = damping.shape
    n = lax.axis_size("gz")
    chunks = rows // HALF
    f32, i32 = jnp.float32, jnp.int32
    edge = -(-3 * secs // 8) * 8
    padded = rows + 2 * HALF
    dma = pltpu.SemaphoreType.DMA
    out = jax.ShapeDtypeStruct(position.shape, f32)
    anyspace = pl.BlockSpec(memory_space=pl.ANY)
    vmem = pl.BlockSpec(memory_space=pltpu.VMEM)
    return pl.pallas_call(
        functools.partial(kernel, n),
        out_shape=(out, out),
        in_specs=[anyspace] * 6 + [pl.BlockSpec(memory_space=pltpu.SMEM)],
        out_specs=(vmem, vmem),
        scratch_shapes=[
            pltpu.VMEM((OPS, 2, secs, padded, cols), f32),
            pltpu.VMEM((OPS, 2, secs, rows, cols), f32),
            pltpu.VMEM((OPS, 3, secs, rows, cols), f32),
            pltpu.VMEM((OPS, 3, secs, rows, cols), f32),
            pltpu.VMEM((OPS + 1, edge, cols), f32),
            pltpu.VMEM((OPS + 1, edge, cols), f32),
            pltpu.VMEM((8, 128), f32),
            pltpu.VMEM((n - 1, 8, 128), f32),
            pltpu.VMEM(gaps.shape, f32),
            pltpu.VMEM(weights.shape, f32),
            pltpu.VMEM(deltas.shape, i32),
            pltpu.VMEM(springs.shape, i32),
            pltpu.VMEM(damping.shape, f32),
            pltpu.VMEM((secs, padded, cols), f32),
            pltpu.VMEM(damping.shape, f32),
            pltpu.VMEM(damping.shape, f32),
            pltpu.VMEM(damping.shape, f32),
            pltpu.VMEM(position.shape, f32),
            dma((6,)),
            dma((OPS, chunks)), dma((OPS, chunks)),
            dma((OPS, chunks)), dma((OPS, chunks)),
            dma((OPS + 1,)), dma((OPS + 1,)),
            dma((n - 1,)), dma((n - 1,)),
        ],
        compiler_params=pltpu.CompilerParams(
            collective_id=0, has_side_effects=True, vmem_limit_bytes=67043328
        ),
    )(position, gaps, weights, deltas, springs, damping, stiffness)


def solution(mesh):
    return jax.shard_map(
        body,
        mesh=mesh,
        in_specs=(
            P(None, "gz", "ta", None),
            P(None, None, "gz", "ta", None),
            P(None, "gz", "ta", None),
            P(None, "gz", "ta", None),
            P(None, "gz", "ta", None),
            P("gz", "ta", None),
            P(None, "gz"),
        ),
        out_specs=(P(None, "gz", "ta", None), P(None, "gz", "ta", None)),
        check_vma=False,
    )
```
